32 devices in a mesh: graph: 16 (over z, y, core), chan: 2 (over x).
Axes of the slice: x: 2, y: 2, z: 4, core: 2. Of those that a mesh axis runs over, the one named last changes fastest.
Arguments:
- embed: bfloat16 [25, 512, 2048], P(None, 'chan', 'graph'), may hold values from -200 to 200
- gain: float32 [5, 512], P(None, 'chan'), may hold values from 0.25 to 1.75
- w_zero: bfloat16 [5, 512, 2560], P(None, 'chan'), may hold values from -0.125 to 0.125
- w_one: bfloat16 [2, 4, 512, 2048], P(None, None, 'chan'), may hold values from -0.125 to 0.125
- w_two: bfloat16 [2, 3, 512, 1536], P(None, None, 'chan'), may hold values from -0.15625 to 0.15625
- rot_table: float32 [19, 25, 256], replicated, may hold values from -1 to 1, as said below
- face_atoms: int32 [512], P('graph'), may hold values from 0 to 127, as said below
- edge_source: int32 [2048], P('graph'), may hold values from 0 to 159
- edge_target: int32 [2048], P('graph'), may hold values from 0 to 127
- rot_index: int32 [2048], P('graph'), may hold values from 0 to 255
- edge_weight: float32 [2048], P('graph'), may hold values from 0.2 to 1
- cotangent: bfloat16 [25, 512, 2048], P(None, 'chan', 'graph'), may hold values from -1.5 to 1.5
Outputs:
- update: bfloat16 [25, 512, 2048], P(None, 'chan', 'graph')
- grad_embed: bfloat16 [25, 512, 2048], P(None, 'chan', 'graph')
- grad_zero: float32 [5, 512, 2560], P(None, 'chan', 'graph')
- grad_one: float32 [2, 4, 512, 2048], P(None, None, 'chan', 'graph')
- grad_two: float32 [2, 3, 512, 1536], P(None, None, 'chan', 'graph')
The draws below stay inside these ranges and needn't reach their ends.
Inputs may be any that keep to these rules, and one draw needn't show every extreme that they name: `rot_table`: for every rotation, frame row (m, l) is nonzero only on the 2l + 1 coefficients of degree l, where it is row l + m of an orthogonal (2l + 1)-square matrix shared by the rows of that degree; the degree-0 entry is 1. `face_atoms`: block b holds 32 distinct atom indices counted from the first atom of block b: the first 16 lie at the face toward block b - 1, the last 16 at the face toward block b + 1. `edge_source`: read as in the step that defines src. `edge_target`: counted from the first atom of the edge's block.
All inputs are finite; a program needn't handle non-finite values.
Results may differ from the reference program's by a relative error of at most 0.0062.
Values may be sent and summed in bfloat16 or wider, within the bound.
A program may use at most 192 MiB of HBM per device.

```python
import math
import jax
import jax.numpy as jnp
from jax import lax

C = 512
ATOM_DEV = 128
HALO = 16
EDGE_DEV = 128
ROTS = 256
ATOMS = 2048
EDGES = 2048
FACES = 512
N_GRAPH = 16


FRAME = ((0, 0), (1, 0), (2, 0), (3, 0), (4, 0), (1, 1), (2, 1), (3, 1), (4, 1), (1, -1), (2, -1), (3, -1), (4, -1), (2, 2), (3, 2), (4, 2), (2, -2), (3, -2), (4, -2))


def draw_embed(key, part):
    keys = jax.random.split(key, 4)
    ramp = jnp.arange(C, dtype=jnp.float32) / C - 0.5
    channel_scale = jnp.exp(math.log(10.0) * ramp) * jax.random.uniform(keys[1], (C,), jnp.float32, 0.7, 1.4)
    atom_scale = jnp.exp(jax.random.uniform(keys[2], (ATOMS,), jnp.float32, math.log(0.3), math.log(3.0)))
    raw = jnp.clip(jax.random.normal(keys[0], (25, C, ATOMS), jnp.float32), -6.0, 6.0)
    values = raw * channel_scale[None, :, None] * atom_scale[None, None, :]
    return jnp.clip(values, -200.0, 200.0).astype(jnp.bfloat16)


def reflect_block(key, size):
    matrix = jnp.broadcast_to(jnp.eye(size, dtype=jnp.float32), (ROTS, size, size))
    for index in range(size):
        vector = jax.random.normal(jax.random.fold_in(key, index), (ROTS, size), jnp.float32)
        vector = vector / jnp.sqrt(jnp.sum(vector * vector, axis=1, keepdims=True) + 1e-12)
        folded = jnp.einsum('rj,rjk->rk', vector, matrix)
        matrix = matrix - 2.0 * vector[:, :, None] * folded[:, None, :]
    return matrix


def draw_rot_table(key, part):
    blocks = [jnp.ones((ROTS, 1, 1), jnp.float32)]
    for degree in range(1, 5):
        blocks.append(reflect_block(jax.random.fold_in(key, 100 + degree), 2 * degree + 1))
    lines = []
    for pair in FRAME:
        degree = pair[0]
        line = jnp.zeros((ROTS, 25), jnp.float32)
        line = line.at[:, degree * degree:(degree + 1) * (degree + 1)].set(blocks[degree][:, degree + pair[1], :])
        lines.append(line)
    table = jnp.stack(lines, axis=0)
    return jnp.transpose(table, (0, 2, 1))


def draw_face_atoms(key, part):
    count = FACES // (2 * HALO)
    keys = jax.random.split(key, count)
    picks = jax.vmap(lambda single: jax.random.permutation(single, ATOM_DEV)[:2 * HALO])(keys)
    return picks.reshape(FACES).astype(jnp.int32)


def with_ends(entries, own_key, low, largest):
    longest = entries.shape.index(max(entries.shape))
    spots = []
    for shift in (0, 1):
        where = [jax.random.randint(jax.random.fold_in(own_key, axis), (), 0, length) for axis, length in enumerate(entries.shape)]
        where[longest] = (where[longest] + shift) % entries.shape[longest]
        spots.append(tuple(where))
    return entries.at[spots[0]].set(low).at[spots[1]].set(largest)


def steps_of(own_key, extent, shards, low, high):
    def one(axis_at, blocks):
        heights = jax.random.uniform(jax.random.fold_in(jax.random.fold_in(own_key, 6), axis_at), (blocks,), jnp.float32, low / len(shards), high / len(shards))
        return jnp.repeat(jnp.exp(heights), extent[axis_at] // blocks).reshape((-1,) + (1,) * (len(extent) - axis_at - 1))

    factor_of = one(*shards[0])
    for cut in shards[1:]:
        factor_of = factor_of * one(*cut)
    return factor_of


def normal_values(rng, dims, scale, reach, cuts=(), kind=jnp.bfloat16):
    entries = scale * jax.random.normal(rng, dims, jnp.float32)
    if cuts:
        entries = entries * steps_of(rng, dims, cuts, -0.22, 0.18)
    return jnp.clip(entries, -reach, reach).astype(kind)


def setup_inputs(seed: int = 0) -> dict:
    splits = jax.random.split(jax.random.key(seed), 13)
    embed = draw_embed(jax.random.fold_in(splits[12], 71), 0)
    gain = jnp.clip(1.0 + 0.15 * jax.random.normal(splits[1], (5, C), jnp.float32), 0.25, 1.75)
    w_zero = normal_values(splits[2], (5, C, 5 * C), (5 * C) ** -0.5, 0.125, ((1, 2),))
    w_one = normal_values(splits[3], (2, 4, C, 4 * C), (4 * C) ** -0.5, 0.125, ((2, 2),))
    w_two = normal_values(splits[4], (2, 3, C, 3 * C), (3 * C) ** -0.5, 0.15625, ((2, 2),))
    rot_table = draw_rot_table(jax.random.fold_in(splits[12], 71), 0)
    face_atoms = draw_face_atoms(jax.random.fold_in(splits[12], 71), 0)
    edge_source = with_ends(jax.random.randint(splits[7], (EDGES,), 0, ATOM_DEV + 2 * HALO), jax.random.fold_in(splits[7], 1), 0, (ATOM_DEV + 2 * HALO) - 1).astype(jnp.int32)
    edge_target = with_ends(jax.random.randint(splits[8], (EDGES,), 0, ATOM_DEV), jax.random.fold_in(splits[8], 1), 0, ATOM_DEV - 1).astype(jnp.int32)
    rot_index = with_ends(jax.random.randint(splits[9], (EDGES,), 0, ROTS), jax.random.fold_in(splits[9], 1), 0, ROTS - 1).astype(jnp.int32)
    edge_weight = jnp.clip(jnp.exp(math.log(1.0) - 1.609438 * jax.random.uniform(splits[10], (EDGES,), jnp.float32) ** steps_of(splits[10], (EDGES,), ((0, 16),), -0.2, 0.2)), 0.2, 1.0)
    cotangent = normal_values(splits[11], (25, C, ATOMS), 0.25, 1.5, ((1, 2), (2, 16)))
    return {"embed": embed, "gain": gain, "w_zero": w_zero, "w_one": w_one, "w_two": w_two, "rot_table": rot_table, "face_atoms": face_atoms, "edge_source": edge_source, "edge_target": edge_target, "rot_index": rot_index, "edge_weight": edge_weight, "cotangent": cotangent}


EPSILON = 1e-06
HIGHEST = lax.Precision.HIGHEST
FRAME = ((0, 0), (1, 0), (2, 0), (3, 0), (4, 0), (1, 1), (2, 1), (3, 1), (4, 1), (1, -1), (2, -1), (3, -1), (4, -1), (2, 2), (3, 2), (4, 2), (2, -2), (3, -2), (4, -2))

def gain_rows(gain):
    pieces = [jnp.broadcast_to(gain[degree:degree + 1], (2 * degree + 1, gain.shape[1])) for degree in range(5)]
    return jnp.concatenate(pieces, axis=0)

def product(left, right):
    return jnp.dot(left, right, preferred_element_type=jnp.float32)

def across(left, right):
    return lax.dot_general(left, right, (((0,), (0,)), ((), ())), preferred_element_type=jnp.float32)

def outer(left, right):
    return lax.dot_general(left, right, (((1,), (1,)), ((), ())), preferred_element_type=jnp.float32)

def stack_frame(parts, width, edges):
    row_counts = (5, 4, 4, 3, 3)
    return jnp.concatenate([part.reshape(rows, width, edges) for part, rows in zip(parts, row_counts)], axis=0)

def mix_part(w_zero, w_one, w_two, piece, start):
    count = piece.shape[1]
    edges = piece.shape[2]
    outputs = w_zero.shape[1]

    def columns(weight, blocks):
        shaped = weight.reshape(blocks * outputs, blocks, weight.shape[-1] // blocks)
        return lax.dynamic_slice_in_dim(shaped, start, count, 2).reshape(blocks * outputs, blocks * count)

    def frame_rows(first, blocks):
        return piece[first:first + blocks].reshape(blocks * count, edges)
    parts = [product(columns(w_zero, 5), frame_rows(0, 5))]
    for weights, first, blocks in ((w_one, 5, 4), (w_two, 13, 3)):
        real_part = columns(weights[0], blocks)
        imag_part = columns(weights[1], blocks)
        plus = frame_rows(first, blocks)
        minus = frame_rows(first + blocks, blocks)
        parts.append(product(real_part, plus) - product(imag_part, minus))
        parts.append(product(real_part, minus) + product(imag_part, plus))
    return tuple(parts)

def mix_backward(w_zero, w_one, w_two, grads, frame):
    outputs = grads.shape[1]
    width = frame.shape[1]
    edges = grads.shape[2]

    def grad_rows(first, blocks):
        return grads[first:first + blocks].reshape(blocks * outputs, edges)

    def frame_rows(first, blocks):
        return frame[first:first + blocks].reshape(blocks * width, edges)
    zero_weight = w_zero.reshape(5 * outputs, 5 * width)
    grad_first = grad_rows(0, 5)
    back = [across(zero_weight, grad_first)]
    weight_zero = outer(grad_first, frame_rows(0, 5)).reshape(5, outputs, 5 * width)
    pairs = []
    for weights, first, blocks in ((w_one, 5, 4), (w_two, 13, 3)):
        real_part = weights[0].reshape(blocks * outputs, blocks * width)
        imag_part = weights[1].reshape(blocks * outputs, blocks * width)
        grad_plus = grad_rows(first, blocks)
        grad_minus = grad_rows(first + blocks, blocks)
        frame_plus = frame_rows(first, blocks)
        frame_minus = frame_rows(first + blocks, blocks)
        back.append(across(real_part, grad_plus) + across(imag_part, grad_minus))
        back.append(across(real_part, grad_minus) - across(imag_part, grad_plus))
        real_grad = outer(grad_plus, frame_plus) + outer(grad_minus, frame_minus)
        imag_grad = outer(grad_minus, frame_plus) - outer(grad_plus, frame_minus)
        pairs.append(jnp.stack([real_grad.reshape(blocks, outputs, blocks * width), imag_grad.reshape(blocks, outputs, blocks * width)]))
    return (stack_frame(back, width, edges), weight_zero, pairs[0], pairs[1])

def reference(embed, gain, w_zero, w_one, w_two, rot_table, face_atoms, edge_source, edge_target, rot_index, edge_weight, cotangent):
    values = embed.astype(jnp.float32)
    gains = gain_rows(gain)
    inverse = lax.rsqrt(lax.optimization_barrier(jnp.sum(values * values, axis=(0, 1))) / (25 * C) + EPSILON)
    normed = (values * inverse[None, None, :] * gains[:, :, None]).astype(jnp.bfloat16)
    positions = jnp.arange(ATOM_DEV, dtype=jnp.int32)

    def shard_step(carry, shard):
        update, grad_normed, grad_zero, grad_one, grad_two = carry
        left = (shard - 1) % N_GRAPH
        right = (shard + 1) % N_GRAPH
        from_left = lax.dynamic_slice_in_dim(face_atoms, left * (2 * HALO) + HALO, HALO)
        from_right = lax.dynamic_slice_in_dim(face_atoms, right * (2 * HALO), HALO)
        lookup = jnp.concatenate([shard * ATOM_DEV + positions, left * ATOM_DEV + from_left, right * ATOM_DEV + from_right]).astype(jnp.int32)
        first = (shard * EDGE_DEV).astype(jnp.int32)
        sources = lookup[lax.dynamic_slice_in_dim(edge_source, first, EDGE_DEV)]
        targets = (shard * ATOM_DEV + lax.dynamic_slice_in_dim(edge_target, first, EDGE_DEV)).astype(jnp.int32)
        rotations = jnp.take(rot_table, lax.dynamic_slice_in_dim(rot_index, first, EDGE_DEV), axis=2)
        scale = lax.dynamic_slice_in_dim(edge_weight, first, EDGE_DEV)
        gathered = jnp.take(normed, sources, axis=2).astype(jnp.float32)
        frame = jnp.einsum('jke,kce->jce', rotations, gathered, precision=HIGHEST).astype(jnp.bfloat16)
        mixed = stack_frame(mix_part(w_zero, w_one, w_two, frame, 0), C, EDGE_DEV)
        message = jnp.einsum('jke,jce->kce', rotations, mixed * scale[None, None, :], precision=HIGHEST).astype(jnp.bfloat16)
        update = update.at[:, :, targets].add(message.astype(jnp.float32))
        arriving = jnp.take(cotangent, targets, axis=2).astype(jnp.float32)
        grads = (jnp.einsum('jke,kce->jce', rotations, arriving, precision=HIGHEST) * scale[None, None, :]).astype(jnp.bfloat16)
        back, part_zero, part_one, part_two = mix_backward(w_zero, w_one, w_two, grads, frame)
        spread = jnp.einsum('jke,jce->kce', rotations, back, precision=HIGHEST)
        grad_normed = grad_normed.at[:, :, sources].add(spread)
        return ((update, grad_normed, grad_zero + part_zero, grad_one + part_one, grad_two + part_two), None)
    start = (jnp.zeros((25, C, ATOMS), jnp.float32), jnp.zeros((25, C, ATOMS), jnp.float32), jnp.zeros((5, C, 5 * C), jnp.float32), jnp.zeros((2, 4, C, 4 * C), jnp.float32), jnp.zeros((2, 3, C, 3 * C), jnp.float32))
    final, unused = lax.scan(shard_step, start, jnp.arange(N_GRAPH, dtype=jnp.int32))
    update, grad_normed, grad_zero, grad_one, grad_two = final
    tally = lax.optimization_barrier(jnp.sum(values * gains[:, :, None] * grad_normed, axis=(0, 1)))
    grad_embed = (inverse[None, None, :] * gains[:, :, None] * grad_normed - values * (inverse ** 3 * tally / (25 * C))[None, None, :]).astype(jnp.bfloat16)
    return (update.astype(jnp.bfloat16), grad_embed, grad_zero, grad_one, grad_two)
```

```python
import functools

import jax
import jax.numpy as jnp
from jax import lax
from jax.experimental import pallas as pl
from jax.experimental.pallas import tpu as pltpu
from jax.sharding import PartitionSpec as P


EPSILON = 1e-06
HIGHEST = lax.Precision.HIGHEST
FRAME = (
    (0, 0),
    (1, 0),
    (2, 0),
    (3, 0),
    (4, 0),
    (1, 1),
    (2, 1),
    (3, 1),
    (4, 1),
    (1, -1),
    (2, -1),
    (3, -1),
    (4, -1),
    (2, 2),
    (3, 2),
    (4, 2),
    (2, -2),
    (3, -2),
    (4, -2),
)


def gain_rows(gain):
    pieces = [
        jnp.broadcast_to(gain[degree : degree + 1], (2 * degree + 1, gain.shape[1]))
        for degree in range(5)
    ]
    return jnp.concatenate(pieces, axis=0)


def product(left, right):
    return jnp.dot(left, right, preferred_element_type=jnp.float32)


def across(left, right):
    return lax.dot_general(
        left, right, (((0,), (0,)), ((), ())), preferred_element_type=jnp.float32
    )


def contract(left, right):
    return lax.dot_general(left, right, (((2,), (1,)), ((), ())), preferred_element_type=jnp.float32)


def frames_kernel(*refs):
    pairs, (rotations, scale, out) = refs[:-3], refs[-3:]
    count, width = pairs[0].shape[0], pairs[0].shape[1]
    total = None
    for values, picks in zip(pairs[0::2], pairs[1::2]):
        part = product(values[...].reshape(count * width, values.shape[2]), picks[...])
        total = part if total is None else total + part
    total = total.reshape(count, width, total.shape[1])
    for row, (degree, _) in enumerate(FRAME):
        first = degree * degree
        entry = row * count + first
        line = rotations[entry : entry + 1, :] * total[first]
        for step in range(1, 2 * degree + 1):
            entry = row * count + first + step
            line = line + rotations[entry : entry + 1, :] * total[first + step]
        out[row] = (line * scale[...]).astype(out.dtype)


def to_frames(pairs, rotations, scale):
    count, local = pairs[0][0].shape[0], pairs[0][0].shape[1]
    edges = scale.shape[1]
    block = min(64, local)
    operands, specs = [], []
    for values, picks in pairs:
        operands += [values, picks]
        specs.append(pl.BlockSpec((count, block, values.shape[2]), lambda i: (0, i, 0)))
        specs.append(pl.BlockSpec(picks.shape, lambda i: (0, 0)))
    for whole in (rotations, scale):
        operands.append(whole)
        specs.append(pl.BlockSpec(whole.shape, lambda i: (0, 0)))
    return pl.pallas_call(
        frames_kernel,
        grid=(local // block,),
        in_specs=specs,
        out_specs=pl.BlockSpec((len(FRAME), block, edges), lambda i: (0, i, 0)),
        out_shape=jax.ShapeDtypeStruct((len(FRAME), local, edges), jnp.bfloat16),
        compiler_params=pltpu.CompilerParams(dimension_semantics=("arbitrary",)),
    )(*operands)


def atoms_kernel(count, values, rotations, scale, *refs):
    picks, outs, held = refs[: len(refs) // 2], refs[len(refs) // 2 : -1], refs[-1]
    width, edges = values.shape[1], values.shape[2]
    for degree in range(5):
        members = [row for row, pair in enumerate(FRAME) if pair[0] == degree]
        lines = [values[row].astype(jnp.float32) * scale[...] for row in members]
        for column in range(degree * degree, (degree + 1) * (degree + 1)):
            total = None
            for row, line in zip(members, lines):
                entry = row * count + column
                term = rotations[entry : entry + 1, :] * line
                total = term if total is None else total + term
            held[column] = total.astype(held.dtype)
    flat = held[...].reshape(count * width, edges)
    for pick, out in zip(picks, outs):
        out[...] = product(flat, pick[...]).reshape(out.shape).astype(out.dtype)


def to_atoms(values, rotations, scale, picks, kinds):
    rows, local, edges = values.shape
    count = rotations.shape[0] // rows
    block = min(64, local)
    whole = lambda i: (0, 0)
    return pl.pallas_call(
        functools.partial(atoms_kernel, count),
        grid=(local // block,),
        in_specs=[
            pl.BlockSpec((rows, block, edges), lambda i: (0, i, 0)),
            pl.BlockSpec(rotations.shape, whole),
            pl.BlockSpec(scale.shape, whole),
        ]
        + [pl.BlockSpec(pick.shape, whole) for pick in picks],
        out_specs=[
            pl.BlockSpec((count, block, pick.shape[1]), lambda i: (0, i, 0)) for pick in picks
        ],
        out_shape=[
            jax.ShapeDtypeStruct((count, local, pick.shape[1]), kind)
            for pick, kind in zip(picks, kinds)
        ],
        scratch_shapes=[pltpu.VMEM((count, block, edges), jnp.bfloat16)],
        compiler_params=pltpu.CompilerParams(dimension_semantics=("arbitrary",)),
    )(values, rotations, scale, *picks)


def swap(block, bit):
    count = lax.axis_size("graph")
    return lax.ppermute(block, "graph", [(i, i ^ bit) for i in range(count)])


def from_beside(faces, width):
    count = lax.axis_size("graph")
    forward = [(i, (i + 1) % count) for i in range(count)]
    backward = [(target, source) for source, target in forward]
    low = lax.ppermute(faces[:, :, width:], "graph", forward)
    high = lax.ppermute(faces[:, :, :width], "graph", backward)
    return jnp.concatenate([low, high], axis=2)


def hot_rows(size, codes):
    return (jnp.arange(size, dtype=jnp.int32)[:, None] == codes[None, :]).astype(jnp.bfloat16)


def hot_columns(codes, size):
    return (codes[:, None] == jnp.arange(size, dtype=jnp.int32)[None, :]).astype(jnp.bfloat16)


def beside(plus, minus, axis=-1):
    return jnp.concatenate([plus, minus], axis=axis)


def mix_forward(weights, frame):
    w_zero, w_one, w_two = weights
    edges = frame.shape[2]
    local = w_zero.shape[1]
    mixed = [
        product(w_zero.reshape(-1, w_zero.shape[2]), frame[:5].reshape(-1, edges)).reshape(
            5, local, edges
        )
    ]
    for weight, first, blocks in ((w_one, 5, 4), (w_two, 13, 3)):
        plus = frame[first : first + blocks].reshape(-1, edges)
        minus = frame[first + blocks : first + 2 * blocks].reshape(-1, edges)
        both = product(weight.reshape(-1, weight.shape[-1]), beside(plus, minus))
        both = both.reshape(2, blocks, local, 2 * edges)
        mixed.append(both[0, :, :, :edges] - both[1, :, :, edges:])
        mixed.append(both[0, :, :, edges:] + both[1, :, :, :edges])
    return jnp.concatenate(mixed, axis=0)


def mix_back(weights, grads, shares):
    w_zero, w_one, w_two = weights
    edges = grads.shape[2]

    def shared(block, blocks):
        shaped = block.reshape(blocks, shares, -1, edges).astype(jnp.bfloat16)
        return jnp.transpose(shaped, (1, 0, 2, 3))

    back = [
        shared(across(w_zero.reshape(-1, w_zero.shape[2]), grads[:5].reshape(-1, edges)), 5)
    ]
    for weight, first, blocks in ((w_one, 5, 4), (w_two, 13, 3)):
        plus = grads[first : first + blocks].reshape(-1, edges)
        minus = grads[first + blocks : first + 2 * blocks].reshape(-1, edges)
        sides = jnp.concatenate([beside(plus, minus), beside(minus, -plus)], axis=0)
        both = across(weight.reshape(-1, weight.shape[-1]), sides)
        back.append(shared(both[:, :edges], blocks))
        back.append(shared(both[:, edges:], blocks))
    return jnp.concatenate(back, axis=1)


def column_frames(frame):
    count = lax.axis_size("graph")
    near = 4
    far = count // near
    edges = frame.shape[2]
    cuts = ((0, 5), (5, 4), (9, 4), (13, 3), (16, 3))
    parts = [
        frame[first : first + blocks].reshape(far, near, -1, edges) for first, blocks in cuts
    ]
    widths = [part.shape[2] for part in parts]
    packed = jnp.concatenate(parts, axis=2)
    mine = lax.axis_index("graph") % near
    frames = []
    for bit in (0, 2, 1, 3):
        target = mine ^ bit
        chunk = lax.dynamic_index_in_dim(packed, target, axis=1, keepdims=False)
        frames.append(swap(chunk, bit) if bit else chunk)
    return frames, widths


def weight_grads(frames, widths, grads_all, local):
    count = lax.axis_size("graph")
    near = 4
    far = count // near
    edges = frames[0].shape[2]
    starts = [sum(widths[:i]) for i in range(5)]
    groups = [[z * near + q for z in range(far)] for q in range(near)]

    def settle(partial):
        return lax.psum_scatter(
            partial.astype(jnp.bfloat16),
            "graph",
            scatter_dimension=0,
            axis_index_groups=groups,
            tiled=False,
        ).astype(jnp.float32)

    def settle_direct(partial):
        partial = partial.astype(jnp.bfloat16)
        place = lax.axis_index("graph") // near
        total = lax.dynamic_index_in_dim(partial, place, axis=0, keepdims=False)
        total = total.astype(jnp.float32)
        for step in range(1, far):
            chunk = lax.dynamic_index_in_dim(partial, (place + step) % far, axis=0, keepdims=False)
            shift = [(i, (i + step * near) % count) for i in range(count)]
            total = total + lax.ppermute(chunk, "graph", shift).astype(jnp.float32)
        return total

    def columns(index):
        return [chunk[:, starts[index] : starts[index] + widths[index]] for chunk in frames]

    left = jnp.concatenate(columns(0), axis=2)
    right = jnp.concatenate([g[:5].reshape(-1, edges) for g in grads_all], axis=1)
    done = settle_direct(contract(left, right))
    results = [jnp.transpose(done).reshape(5, local, widths[0])]
    for index, first, blocks in ((1, 5, 4), (3, 13, 3)):
        plus, minus = columns(index), columns(index + 1)
        real_part = jnp.concatenate([x for pair in zip(plus, minus) for x in pair], axis=2)
        imag_part = jnp.concatenate([x for pair in zip(minus, plus) for x in (-pair[0], pair[1])], axis=2)
        left = jnp.concatenate([real_part, imag_part], axis=1)
        right = jnp.concatenate(
            [
                g[start : start + blocks].reshape(-1, edges)
                for g in grads_all
                for start in (first, first + blocks)
            ],
            axis=1,
        )
        done = settle(contract(left, right))
        done = done.reshape(2, widths[index], blocks * local)
        results.append(jnp.transpose(done, (0, 2, 1)).reshape(2, blocks, local, widths[index]))
    return results


def shards(
    embed,
    gain,
    w_zero,
    w_one,
    w_two,
    rot_table,
    face_atoms,
    edge_source,
    edge_target,
    rot_index,
    edge_weight,
    cotangent,
):
    atoms = embed.shape[2]
    local = embed.shape[1]
    halo = face_atoms.shape[0] // 2
    shares = lax.axis_size("chan")
    channels = local * shares
    weights = (w_zero, w_one, w_two)
    values = embed.astype(jnp.float32)
    gains = gain_rows(gain)
    rows, coefficients, rots = rot_table.shape
    which = (jnp.arange(rots, dtype=jnp.int32)[:, None] == rot_index[None, :]).astype(jnp.float32)
    rotations = jnp.dot(
        rot_table.reshape(rows * coefficients, rots),
        which,
        precision=HIGHEST,
        preferred_element_type=jnp.float32,
    )
    weight_row = edge_weight[None, :]
    ones = jnp.ones_like(weight_row)

    squares = lax.psum(jnp.sum(values * values, axis=(0, 1)), "chan")
    inverse = lax.rsqrt(squares / (25 * channels) + EPSILON)
    normed = (values * inverse[None, None, :] * gains[:, :, None]).astype(jnp.bfloat16)
    flat = normed.reshape(25 * local, atoms)
    faces = product(flat, hot_rows(atoms, face_atoms)).astype(jnp.bfloat16)
    table_end = from_beside(faces.reshape(25, local, 2 * halo), halo)

    grads = to_frames([(cotangent, hot_rows(atoms, edge_target))], rotations, weight_row)
    picks = hot_rows(atoms + 2 * halo, edge_source)
    own = to_frames([(normed, picks[:atoms]), (table_end, picks[atoms:])], rotations, ones)
    own, grads = lax.optimization_barrier((own, grads))
    piece = lax.all_gather(own, "chan", axis=1, tiled=True)

    grads_side = swap(grads, 2)
    pair = swap(jnp.stack([grads, grads_side]), 1)
    grads_all = [grads, grads_side, pair[0], pair[1]]

    back = lax.psum_scatter(
        mix_back(weights, grads, shares), "chan", scatter_dimension=0, tiled=False
    )
    frames, widths = column_frames(piece)
    mixed = mix_forward(weights, piece)
    mixed, frames = lax.optimization_barrier((mixed, frames))
    (update,) = to_atoms(
        mixed, rotations, weight_row, [hot_columns(edge_target, atoms)], [jnp.bfloat16]
    )
    leaving = hot_columns(edge_source, atoms + 2 * halo)
    mine, outward = to_atoms(
        back,
        rotations,
        ones,
        [leaving[:, :atoms], leaving[:, atoms:]],
        [jnp.float32, jnp.bfloat16],
    )
    incoming = from_beside(outward, halo)
    settled = product(incoming.reshape(25 * local, 2 * halo), hot_columns(face_atoms, atoms))
    grad_normed = mine + settled.reshape(25, local, atoms)
    scaled = inverse[None, None, :] * gains[:, :, None] * grad_normed
    tally = lax.psum(jnp.sum(values * scaled, axis=(0, 1)), "chan")
    grad_embed = (
        scaled
        - values * (inverse**2 * tally / (25 * channels))[None, None, :]
    ).astype(jnp.bfloat16)
    grad_zero, grad_one, grad_two = weight_grads(frames, widths, grads_all, local)
    return (update, grad_embed, grad_zero, grad_one, grad_two)


def solution(mesh):
    placed = (
        P(None, "chan", "graph"),
        P(None, "chan"),
        P(None, "chan", None),
        P(None, None, "chan", None),
        P(None, None, "chan", None),
        P(),
        P("graph"),
        P("graph"),
        P("graph"),
        P("graph"),
        P("graph"),
        P(None, "chan", "graph"),
    )
    return jax.shard_map(
        shards,
        mesh=mesh,
        in_specs=placed,
        out_specs=(
            P(None, "chan", "graph"),
            P(None, "chan", "graph"),
            P(None, "chan", "graph"),
            P(None, None, "chan", "graph"),
            P(None, None, "chan", "graph"),
        ),
        check_vma=False,
    )
```

```python
import functools

import jax
import jax.numpy as jnp
from jax import lax
from jax.experimental import pallas as pl
from jax.experimental.pallas import tpu as pltpu
from jax.sharding import PartitionSpec as P


EPSILON = 1e-06
HIGHEST = lax.Precision.HIGHEST
FRAME = (
    (0, 0),
    (1, 0),
    (2, 0),
    (3, 0),
    (4, 0),
    (1, 1),
    (2, 1),
    (3, 1),
    (4, 1),
    (1, -1),
    (2, -1),
    (3, -1),
    (4, -1),
    (2, 2),
    (3, 2),
    (4, 2),
    (2, -2),
    (3, -2),
    (4, -2),
)


def gain_rows(gain):
    pieces = [
        jnp.broadcast_to(gain[degree : degree + 1], (2 * degree + 1, gain.shape[1]))
        for degree in range(5)
    ]
    return jnp.concatenate(pieces, axis=0)


def product(left, right):
    return jnp.dot(left, right, preferred_element_type=jnp.float32)


def across(left, right):
    return lax.dot_general(
        left, right, (((0,), (0,)), ((), ())), preferred_element_type=jnp.float32
    )


def contract(left, right):
    return lax.dot_general(left, right, (((2,), (1,)), ((), ())), preferred_element_type=jnp.float32)


def frames_kernel(*refs):
    pairs, (rotations, scale, out) = refs[:-3], refs[-3:]
    count, width = pairs[0].shape[0], pairs[0].shape[1]
    total = None
    for values, picks in zip(pairs[0::2], pairs[1::2]):
        part = product(values[...].reshape(count * width, values.shape[2]), picks[...])
        total = part if total is None else total + part
    total = total.reshape(count, width, total.shape[1])
    for row, (degree, _) in enumerate(FRAME):
        first = degree * degree
        entry = row * count + first
        line = rotations[entry : entry + 1, :] * total[first]
        for step in range(1, 2 * degree + 1):
            entry = row * count + first + step
            line = line + rotations[entry : entry + 1, :] * total[first + step]
        out[row] = (line * scale[...]).astype(out.dtype)


def to_frames(pairs, rotations, scale):
    count, local = pairs[0][0].shape[0], pairs[0][0].shape[1]
    edges = scale.shape[1]
    block = min(64, local)
    operands, specs = [], []
    for values, picks in pairs:
        operands += [values, picks]
        specs.append(pl.BlockSpec((count, block, values.shape[2]), lambda i: (0, i, 0)))
        specs.append(pl.BlockSpec(picks.shape, lambda i: (0, 0)))
    for whole in (rotations, scale):
        operands.append(whole)
        specs.append(pl.BlockSpec(whole.shape, lambda i: (0, 0)))
    return pl.pallas_call(
        frames_kernel,
        grid=(local // block,),
        in_specs=specs,
        out_specs=pl.BlockSpec((len(FRAME), block, edges), lambda i: (0, i, 0)),
        out_shape=jax.ShapeDtypeStruct((len(FRAME), local, edges), jnp.bfloat16),
        compiler_params=pltpu.CompilerParams(dimension_semantics=("arbitrary",)),
    )(*operands)


def atoms_kernel(count, values, rotations, scale, *refs):
    picks, outs, held = refs[: len(refs) // 2], refs[len(refs) // 2 : -1], refs[-1]
    width, edges = values.shape[1], values.shape[2]
    for degree in range(5):
        members = [row for row, pair in enumerate(FRAME) if pair[0] == degree]
        lines = [values[row].astype(jnp.float32) * scale[...] for row in members]
        for column in range(degree * degree, (degree + 1) * (degree + 1)):
            total = None
            for row, line in zip(members, lines):
                entry = row * count + column
                term = rotations[entry : entry + 1, :] * line
                total = term if total is None else total + term
            held[column] = total.astype(held.dtype)
    flat = held[...].reshape(count * width, edges)
    for pick, out in zip(picks, outs):
        out[...] = product(flat, pick[...]).reshape(out.shape).astype(out.dtype)


def to_atoms(values, rotations, scale, picks, kinds):
    rows, local, edges = values.shape
    count = rotations.shape[0] // rows
    block = min(64, local)
    whole = lambda i: (0, 0)
    return pl.pallas_call(
        functools.partial(atoms_kernel, count),
        grid=(local // block,),
        in_specs=[
            pl.BlockSpec((rows, block, edges), lambda i: (0, i, 0)),
            pl.BlockSpec(rotations.shape, whole),
            pl.BlockSpec(scale.shape, whole),
        ]
        + [pl.BlockSpec(pick.shape, whole) for pick in picks],
        out_specs=[
            pl.BlockSpec((count, block, pick.shape[1]), lambda i: (0, i, 0)) for pick in picks
        ],
        out_shape=[
            jax.ShapeDtypeStruct((count, local, pick.shape[1]), kind)
            for pick, kind in zip(picks, kinds)
        ],
        scratch_shapes=[pltpu.VMEM((count, block, edges), jnp.bfloat16)],
        compiler_params=pltpu.CompilerParams(dimension_semantics=("arbitrary",)),
    )(values, rotations, scale, *picks)


def swap(block, bit):
    count = lax.axis_size("graph")
    return lax.ppermute(block, "graph", [(i, i ^ bit) for i in range(count)])


def from_beside(faces, width):
    count = lax.axis_size("graph")
    forward = [(i, (i + 1) % count) for i in range(count)]
    backward = [(target, source) for source, target in forward]
    low = lax.ppermute(faces[:, :, width:], "graph", forward)
    high = lax.ppermute(faces[:, :, :width], "graph", backward)
    return jnp.concatenate([low, high], axis=2)


def all_channels(own):
    shares = lax.axis_size("chan")
    if shares != 2:
        return lax.all_gather(own, "chan", axis=1, tiled=True)
    other = lax.ppermute(own, "chan", [(0, 1), (1, 0)])
    place = lax.axis_index("chan")
    low = jnp.where(place == 0, own, other)
    high = jnp.where(place == 0, other, own)
    return jnp.concatenate([low, high], axis=1)


def hot_rows(size, codes):
    return (jnp.arange(size, dtype=jnp.int32)[:, None] == codes[None, :]).astype(jnp.bfloat16)


def hot_columns(codes, size):
    return (codes[:, None] == jnp.arange(size, dtype=jnp.int32)[None, :]).astype(jnp.bfloat16)


def beside(plus, minus, axis=-1):
    return jnp.concatenate([plus, minus], axis=axis)


def mix_forward(weights, frame):
    w_zero, w_one, w_two = weights
    edges = frame.shape[2]
    local = w_zero.shape[1]
    mixed = [
        product(w_zero.reshape(-1, w_zero.shape[2]), frame[:5].reshape(-1, edges)).reshape(
            5, local, edges
        )
    ]
    for weight, first, blocks in ((w_one, 5, 4), (w_two, 13, 3)):
        plus = frame[first : first + blocks].reshape(-1, edges)
        minus = frame[first + blocks : first + 2 * blocks].reshape(-1, edges)
        both = product(weight.reshape(-1, weight.shape[-1]), beside(plus, minus))
        both = both.reshape(2, blocks, local, 2 * edges)
        mixed.append(both[0, :, :, :edges] - both[1, :, :, edges:])
        mixed.append(both[0, :, :, edges:] + both[1, :, :, :edges])
    return jnp.concatenate(mixed, axis=0)


def mix_back(weights, grads, shares):
    w_zero, w_one, w_two = weights
    edges = grads.shape[2]

    def shared(block, blocks):
        shaped = block.reshape(blocks, shares, -1, edges).astype(jnp.bfloat16)
        return jnp.transpose(shaped, (1, 0, 2, 3))

    back = [
        shared(across(w_zero.reshape(-1, w_zero.shape[2]), grads[:5].reshape(-1, edges)), 5)
    ]
    for weight, first, blocks in ((w_one, 5, 4), (w_two, 13, 3)):
        plus = grads[first : first + blocks].reshape(-1, edges)
        minus = grads[first + blocks : first + 2 * blocks].reshape(-1, edges)
        sides = jnp.concatenate([beside(plus, minus), beside(minus, -plus)], axis=0)
        both = across(weight.reshape(-1, weight.shape[-1]), sides)
        back.append(shared(both[:, :edges], blocks))
        back.append(shared(both[:, edges:], blocks))
    return jnp.concatenate(back, axis=1)


def column_frames(frame):
    count = lax.axis_size("graph")
    near = 4
    far = count // near
    edges = frame.shape[2]
    cuts = ((0, 5), (5, 4), (9, 4), (13, 3), (16, 3))
    parts = [
        frame[first : first + blocks].reshape(far, near, -1, edges) for first, blocks in cuts
    ]
    widths = [part.shape[2] for part in parts]
    packed = jnp.concatenate(parts, axis=2)
    mine = lax.axis_index("graph") % near
    frames = []
    for bit in (0, 2, 1, 3):
        target = mine ^ bit
        chunk = lax.dynamic_index_in_dim(packed, target, axis=1, keepdims=False)
        frames.append(swap(chunk, bit) if bit else chunk)
    return frames, widths


def weight_grads(frames, widths, grads_all, local, first_done):
    count = lax.axis_size("graph")
    near = 4
    far = count // near
    edges = frames[0].shape[2]
    starts = [sum(widths[:i]) for i in range(5)]
    groups = [[z * near + q for z in range(far)] for q in range(near)]

    def settle(partial):
        return lax.psum_scatter(
            partial.astype(jnp.bfloat16),
            "graph",
            scatter_dimension=0,
            axis_index_groups=groups,
            tiled=False,
        ).astype(jnp.float32)

    def settle_direct(partial):
        partial, _ = lax.optimization_barrier((partial.astype(jnp.bfloat16), first_done))
        place = lax.axis_index("graph") // near
        total = lax.dynamic_index_in_dim(partial, place, axis=0, keepdims=False)
        total = total.astype(jnp.float32)
        for step in range(1, far):
            chunk = lax.dynamic_index_in_dim(partial, (place + step) % far, axis=0, keepdims=False)
            shift = [(i, (i + step * near) % count) for i in range(count)]
            total = total + lax.ppermute(chunk, "graph", shift).astype(jnp.float32)
        return total

    def columns(index):
        return [chunk[:, starts[index] : starts[index] + widths[index]] for chunk in frames]

    left = jnp.concatenate(columns(0), axis=2)
    right = jnp.concatenate([g[:5].reshape(-1, edges) for g in grads_all], axis=1)
    done = settle_direct(contract(left, right))
    results = [jnp.transpose(done).reshape(5, local, widths[0])]
    for index, first, blocks in ((1, 5, 4), (3, 13, 3)):
        plus, minus = columns(index), columns(index + 1)
        real_part = jnp.concatenate([x for pair in zip(plus, minus) for x in pair], axis=2)
        imag_part = jnp.concatenate([x for pair in zip(minus, plus) for x in (-pair[0], pair[1])], axis=2)
        left = jnp.concatenate([real_part, imag_part], axis=1)
        right = jnp.concatenate(
            [
                g[start : start + blocks].reshape(-1, edges)
                for g in grads_all
                for start in (first, first + blocks)
            ],
            axis=1,
        )
        done = settle(contract(left, right))
        done = done.reshape(2, widths[index], blocks * local)
        results.append(jnp.transpose(done, (0, 2, 1)).reshape(2, blocks, local, widths[index]))
    return results


def shards(
    embed,
    gain,
    w_zero,
    w_one,
    w_two,
    rot_table,
    face_atoms,
    edge_source,
    edge_target,
    rot_index,
    edge_weight,
    cotangent,
):
    atoms = embed.shape[2]
    local = embed.shape[1]
    halo = face_atoms.shape[0] // 2
    shares = lax.axis_size("chan")
    channels = local * shares
    weights = (w_zero, w_one, w_two)
    values = embed.astype(jnp.float32)
    gains = gain_rows(gain)
    rows, coefficients, rots = rot_table.shape
    which = (jnp.arange(rots, dtype=jnp.int32)[:, None] == rot_index[None, :]).astype(jnp.float32)
    rotations = jnp.dot(
        rot_table.reshape(rows * coefficients, rots),
        which,
        precision=HIGHEST,
        preferred_element_type=jnp.float32,
    )
    weight_row = edge_weight[None, :]
    ones = jnp.ones_like(weight_row)

    squares = lax.psum(jnp.sum(values * values, axis=(0, 1)), "chan")
    inverse = lax.rsqrt(squares / (25 * channels) + EPSILON)
    normed = (values * inverse[None, None, :] * gains[:, :, None]).astype(jnp.bfloat16)
    flat = normed.reshape(25 * local, atoms)
    faces = product(flat, hot_rows(atoms, face_atoms)).astype(jnp.bfloat16)
    table_end = from_beside(faces.reshape(25, local, 2 * halo), halo)

    grads = to_frames([(cotangent, hot_rows(atoms, edge_target))], rotations, weight_row)
    picks = hot_rows(atoms + 2 * halo, edge_source)
    own = to_frames([(normed, picks[:atoms]), (table_end, picks[atoms:])], rotations, ones)
    own, grads = lax.optimization_barrier((own, grads))
    piece = all_channels(own)

    grads_side = swap(grads, 2)
    pair = swap(jnp.stack([grads, grads_side]), 1)
    grads_all = [grads, grads_side, pair[0], pair[1]]

    back = lax.psum_scatter(
        mix_back(weights, grads, shares), "chan", scatter_dimension=0, tiled=False
    )
    frames, widths = column_frames(piece)
    mixed = mix_forward(weights, piece)
    mixed, frames = lax.optimization_barrier((mixed, frames))
    (update,) = to_atoms(
        mixed, rotations, weight_row, [hot_columns(edge_target, atoms)], [jnp.bfloat16]
    )
    leaving = hot_columns(edge_source, atoms + 2 * halo)
    mine, outward = to_atoms(
        back,
        rotations,
        ones,
        [leaving[:, :atoms], leaving[:, atoms:]],
        [jnp.float32, jnp.bfloat16],
    )
    incoming = from_beside(outward, halo)
    settled = product(incoming.reshape(25 * local, 2 * halo), hot_columns(face_atoms, atoms))
    grad_normed = mine + settled.reshape(25, local, atoms)
    scaled = inverse[None, None, :] * gains[:, :, None] * grad_normed
    tally = lax.psum(jnp.sum(values * scaled, axis=(0, 1)), "chan")
    grad_embed = (
        scaled
        - values * (inverse**2 * tally / (25 * channels))[None, None, :]
    ).astype(jnp.bfloat16)
    grad_zero, grad_one, grad_two = weight_grads(frames, widths, grads_all, local, incoming)
    return (update, grad_embed, grad_zero, grad_one, grad_two)


def solution(mesh):
    placed = (
        P(None, "chan", "graph"),
        P(None, "chan"),
        P(None, "chan", None),
        P(None, None, "chan", None),
        P(None, None, "chan", None),
        P(),
        P("graph"),
        P("graph"),
        P("graph"),
        P("graph"),
        P("graph"),
        P(None, "chan", "graph"),
    )
    return jax.shard_map(
        shards,
        mesh=mesh,
        in_specs=placed,
        out_specs=(
            P(None, "chan", "graph"),
            P(None, "chan", "graph"),
            P(None, "chan", "graph"),
            P(None, None, "chan", "graph"),
            P(None, None, "chan", "graph"),
        ),
        check_vma=False,
    )
```
